32 devices in a mesh: ctx: 32 (over z, y, x, core).
Axes of the slice: x: 2, y: 2, z: 4, core: 2. Of those that a mesh axis runs over, the one named last changes fastest.
Arguments:
- queries: bfloat16 [8192, 768], P('ctx'), may hold values from -16 to 16
- keys: bfloat16 [8192, 768], P('ctx'), may hold values from -16 to 16
- values: bfloat16 [8192, 768], P('ctx'), may hold values from -6 to 6
- offsets: int32 [5, 12], replicated, may hold values from 0 to 31, as said below
Outputs:
- attended: bfloat16 [8192, 768], P('ctx')
The draws below stay inside these ranges and needn't reach their ends.
Inputs may be any that keep to these rules, and one draw needn't show every extreme that they name: offsets[l, h] lies in 0 to min(4 ** l, 32) - 1.
All inputs are finite; a program needn't handle non-finite values.
Results may differ from the reference program's by a relative error of at most 0.0035.
Values may be sent and summed in bfloat16 or wider, within the bound.
A program may use at most 64 MiB of HBM per device.

```python
import jax
import jax.numpy as jnp
from jax import lax

HEADS = 12
HEAD_DIM = 64
LEVELS = 5
TOK_DEV = 256
D = 768
SEQ = 8192
N_CTX = 32


def draw_keys(key, part):
    base = jax.random.normal(jax.random.fold_in(key, 11), (SEQ, D), jnp.float32)
    return jnp.clip(base, -16.0, 16.0).astype(jnp.bfloat16)


def draw_queries(key, part):
    base = jax.random.normal(jax.random.fold_in(key, 13), (SEQ, D), jnp.float32)
    return jnp.clip(base, -16.0, 16.0).astype(jnp.bfloat16)


def draw_offsets(key, part):
    spans = jnp.minimum(4 ** jnp.arange(LEVELS, dtype=jnp.int32), N_CTX)
    raw = jax.random.randint(jax.random.fold_in(key, 17), (LEVELS, HEADS), 0, 1 << 20)
    return (raw % spans[:, None]).astype(jnp.int32)


def levels(key, extent, split, smallest, top_value):
    def one(axis_at, shards_of):
        heights = jax.random.uniform(jax.random.fold_in(jax.random.fold_in(key, 6), axis_at), (shards_of,), jnp.float32, smallest / len(split), top_value / len(split))
        return jnp.repeat(jnp.exp(heights), extent[axis_at] // shards_of).reshape((-1,) + (1,) * (len(extent) - axis_at - 1))

    level = one(*split[0])
    for cut in split[1:]:
        level = level * one(*cut)
    return level


def scatter_about(stream_key, dims, spread, most, cuts=(), held_as=jnp.bfloat16):
    drawn = jax.random.normal(stream_key, dims, jnp.float32) * spread
    if len(cuts) > 0:
        drawn = levels(stream_key, dims, cuts, -0.22, 0.18) * drawn
    return jnp.clip(drawn, min=-most, max=most).astype(held_as)


def setup_inputs(seed: int = 0) -> dict:
    seeds = jax.random.split(jax.random.key(seed), 5)
    queries = draw_queries(jax.random.fold_in(seeds[4], 71), 0)
    keys = draw_keys(jax.random.fold_in(seeds[4], 71), 0)
    values = scatter_about(seeds[2], (SEQ, D), 1.0, 6.0, ((0, 32),))
    offsets = draw_offsets(jax.random.fold_in(seeds[4], 71), 0)
    return {"queries": queries, "keys": keys, "values": values, "offsets": offsets}


def attend_rows(query_rows, key_rows, value_rows, query_pos, key_pos, heads, scale):
    rows = query_rows.shape[0]
    cols = key_rows.shape[0]
    head_size = query_rows.shape[1] // heads
    query_heads = query_rows.reshape(rows, heads, head_size)
    key_heads = key_rows.reshape(cols, heads, head_size)
    value_heads = value_rows.reshape(cols, heads, head_size)
    allowed = key_pos[None, :] <= query_pos[:, None]
    scores = jnp.einsum("qhd,khd->hqk", query_heads, key_heads, preferred_element_type=jnp.float32) * scale
    scores = jnp.where(allowed[None], scores, -1e30)
    peak = jnp.max(scores, axis=2)
    weights = jnp.where(allowed[None], jnp.exp(scores - peak[:, :, None]), 0.0)
    totals = jnp.sum(weights, axis=2)
    result = jnp.einsum("hqk,khd->qhd", weights.astype(jnp.bfloat16), value_heads, preferred_element_type=jnp.float32)
    return result / totals.T[:, :, None], (peak + jnp.log(totals)).T


def causal_blocks(query_rows, key_rows, value_rows, heads, scale):
    length = query_rows.shape[0]
    block = min(512, length)
    outputs = []
    sums = []
    for number in range(length // block):
        query_pos = jnp.arange(number * block, (number + 1) * block, dtype=jnp.int32)
        key_pos = jnp.arange((number + 1) * block, dtype=jnp.int32)
        result, lse_part = attend_rows(query_rows[number * block:(number + 1) * block], key_rows[:(number + 1) * block], value_rows[:(number + 1) * block], query_pos, key_pos, heads, scale)
        outputs.append(result)
        sums.append(lse_part)
    return jnp.concatenate(outputs, 0), jnp.concatenate(sums, 0)


def select_rows(source, offset_row, group, heads):
    count = source.shape[0]
    head_size = source.shape[1] // heads
    shaped = source.reshape(count // group, group, heads, head_size)
    hit = jnp.arange(group, dtype=jnp.int32)[:, None] == offset_row.astype(jnp.int32)[None, :]
    picked = jnp.sum(jnp.where(hit[None, :, :, None], shaped, jnp.zeros((), source.dtype)), axis=1)
    return picked.astype(source.dtype).reshape(count // group, heads * head_size)


def merge_levels(base_out, base_lse, extras):
    rows_all, heads, head_size = base_out.shape
    best = base_lse
    numer = base_out
    denom = jnp.ones(base_lse.shape, jnp.float32)
    for level_out, level_lse, offset_row, group in extras:
        rows = level_out.shape[0]
        hit = jnp.arange(group, dtype=jnp.int32)[:, None] == offset_row.astype(jnp.int32)[None, :]
        best_g = best.reshape(rows, group, heads)
        lse_g = jnp.where(hit[None], level_lse[:, None], -1e30)
        newest = jnp.maximum(best_g, lse_g)
        keep_old = jnp.exp(best_g - newest)
        take_new = jnp.exp(lse_g - newest)
        numer = (numer.reshape(rows, group, heads, head_size) * keep_old[..., None] + level_out[:, None] * take_new[..., None]).reshape(rows_all, heads, head_size)
        denom = (denom.reshape(rows, group, heads) * keep_old + take_new).reshape(rows_all, heads)
        best = newest.reshape(rows_all, heads)
    merged = numer / denom[..., None]
    return merged.reshape(rows_all, -1).astype(jnp.bfloat16)


def reference(queries, keys, values, offsets):
    scale = HEAD_DIM ** -0.5
    level_outs = []
    level_lses = []
    for height in range(LEVELS):
        group = min(4 ** height, N_CTX)
        segments = SEQ // (TOK_DEV * group)
        picked_q = select_rows(queries, offsets[height], group, HEADS).reshape(segments, TOK_DEV, D)
        picked_k = select_rows(keys, offsets[height], group, HEADS).reshape(segments, TOK_DEV, D)
        picked_v = select_rows(values, offsets[height], group, HEADS).reshape(segments, TOK_DEV, D)
        outs, lses = lax.map(lambda triple: causal_blocks(triple[0], triple[1], triple[2], HEADS, scale), (picked_q, picked_k, picked_v))
        rows = TOK_DEV // group
        level_outs.append(outs.reshape(N_CTX, rows, HEADS, HEAD_DIM))
        level_lses.append(lses.reshape(N_CTX, rows, HEADS))

    def per_shard(shard_data):
        shard_outs, shard_lses = shard_data
        extras = []
        for height in range(1, LEVELS):
            extras.append((shard_outs[height], shard_lses[height], offsets[height], min(4 ** height, N_CTX)))
        return merge_levels(shard_outs[0], shard_lses[0], extras)

    shards = lax.map(per_shard, (tuple(level_outs), tuple(level_lses)))
    return shards.reshape(SEQ, D)
```

```python
import functools

import jax
import jax.numpy as jnp
from jax import lax
from jax.experimental import pallas as pl
from jax.experimental.pallas import tpu as pltpu
from jax.sharding import PartitionSpec as P

MESH = pl.DeviceIdType.MESH


def plan_of(levels, count, tokens, heads):
    plan = []
    shift = 0
    for height in range(1, levels):
        group = min(4**height, count)
        per = -(-heads // group)
        plan.append((height, group, tokens // group, per, shift % group))
        if per == 1:
            shift += heads
    return plan


def halves(shape):
    return lax.broadcasted_iota(jnp.int32, shape, 1) < shape[1] // 2


def swap_halves(value):
    return pltpu.roll(value.astype(jnp.float32), value.shape[1] // 2, 1)


def causal_unit(query, key, value):
    tokens = query.shape[0]
    half = tokens // 2
    outs, peaks = [], []
    for start in (0, half):
        end = start + half
        scores = lax.dot_general(
            query[start:end],
            key[:end],
            (((1,), (1,)), ((), ())),
            preferred_element_type=jnp.float32,
        )
        rows = lax.broadcasted_iota(jnp.int32, scores.shape, 0) + start
        cols = lax.broadcasted_iota(jnp.int32, scores.shape, 1)
        scores = jnp.where(cols <= rows, scores, -1e30)
        peak = jnp.max(scores, axis=1, keepdims=True)
        weights = jnp.exp(scores - peak).astype(jnp.bfloat16)
        outs.append(jnp.dot(weights, value[:end], preferred_element_type=jnp.float32))
        peaks.append(peak)
    return jnp.concatenate(outs, 0), jnp.concatenate(peaks, 0)


def exchange_kernel(plan, heads, scale, offs, q_ref, k_ref, v_ref, out_ref, *scratch):
    number = len(plan)
    stage = scratch[:number]
    inbox = scratch[number : 2 * number]
    outbox = scratch[2 * number : 3 * number]
    back = scratch[3 * number : 4 * number]
    numer, total, peaks, send_sem, recv_sem, ret_send, ret_recv = scratch[4 * number :]
    tokens = q_ref.shape[0]
    pair = 2 * (q_ref.shape[1] // heads)
    pairs = heads // 2
    me = lax.axis_index("ctx")
    count = lax.axis_size("ctx")

    barrier = pltpu.get_barrier_semaphore()

    def greet(step, carry):
        other = lax.rem(me + step, count)
        pl.semaphore_signal(barrier, inc=1, device_id=(other,), device_id_type=MESH)
        return carry

    lax.fori_loop(1, count, greet, 0)

    picked = sum(rows for _, _, rows, _, _ in plan)
    row_id = lax.broadcasted_iota(jnp.int32, (picked, tokens), 0)
    col_id = lax.broadcasted_iota(jnp.int32, (picked, tokens), 1)
    low_p = halves((picked, pair))

    def pick(p, carry):
        cols = pl.ds(pl.multiple_of(p * pair, pair), pair)
        packed = jnp.concatenate([q_ref[:, cols], k_ref[:, cols], v_ref[:, cols]], 1)
        for side in range(2):
            head = 2 * p + side
            first = 0
            target = jnp.zeros((picked, tokens), jnp.int32)
            for height, group, rows, _, _ in plan:
                here = (row_id - first) * group + offs[height, head]
                target = here if first == 0 else jnp.where(row_id < first, target, here)
                first += rows
            hit = jnp.where(col_id == target, 1.0, 0.0).astype(jnp.bfloat16)
            got = jnp.dot(hit, packed, preferred_element_type=jnp.float32)
            query, key, value = got[:, :pair], got[:, pair : 2 * pair], got[:, 2 * pair :]
            if side == 0:
                key = swap_halves(key)
            else:
                query, value = swap_halves(query), swap_halves(value)
            left = jnp.where(low_p, query * scale, key)
            right = jnp.where(low_p, value, 1.0)
            both = jnp.concatenate([left, right], 1)
            first = 0
            for at, (_, _, rows, _, _) in enumerate(plan):
                stage[at][head] = both[first : first + rows].astype(stage[at].dtype)
                first += rows
        return carry

    lax.fori_loop(0, pairs, pick, 0)
    pl.semaphore_wait(barrier, count - 1)

    def place(entry, head):
        _, group, _, per, shift = entry
        where = lax.rem(shift + head // per, group)
        mine = lax.rem(me, group)
        return me - mine + where, where == mine, mine, head % per

    def sending(at, head):
        owner, _, mine, slot = place(plan[at], head)
        return pltpu.make_async_remote_copy(
            src_ref=stage[at].at[head],
            dst_ref=inbox[at].at[slot, mine],
            send_sem=send_sem.at[at, head],
            recv_sem=recv_sem.at[at, slot],
            device_id=(owner,),
            device_id_type=MESH,
        )

    order = list(range(number))[::-1]
    for at in order:

        def push(head, carry, at=at):
            _, own, mine, slot = place(plan[at], head)

            @pl.when(jnp.logical_not(own))
            def _():
                sending(at, head).start()

            @pl.when(own)
            def _():
                inbox[at][slot, mine] = stage[at][head]

            return carry

        lax.fori_loop(0, heads, push, 0)

    low = halves((tokens, pair))

    def base(p, carry):
        cols = pl.ds(pl.multiple_of(p * pair, pair), pair)
        query = q_ref[:, cols].astype(jnp.float32) * scale
        key = k_ref[:, cols]
        value = v_ref[:, cols].astype(jnp.float32)
        got = []
        for side in range(2):
            mask = low if side == 0 else jnp.logical_not(low)
            got.append(
                causal_unit(
                    jnp.where(mask, query, 0.0).astype(jnp.bfloat16),
                    key,
                    jnp.where(mask, value, 1.0).astype(jnp.bfloat16),
                )
            )
        numer[:, cols] = jnp.where(low, got[0][0], got[1][0])
        total[:, cols] = swap_halves(jnp.where(low, got[1][0], got[0][0]))
        peaks[:, cols] = jnp.where(low, got[0][1], got[1][1])
        return carry

    lax.fori_loop(0, pairs, base, 0)

    lane = lax.broadcasted_iota(jnp.int32, (tokens, pair), 1)
    mid_lane = pair // 2

    def returning(at, slot, head, there):
        _, group, _, _, _ = plan[at]
        mine = lax.rem(me, group)
        return pltpu.make_async_remote_copy(
            src_ref=outbox[at].at[slot, there],
            dst_ref=back[at].at[head],
            send_sem=ret_send.at[at, slot],
            recv_sem=ret_recv.at[at, head],
            device_id=(me - mine + there,),
            device_id_type=MESH,
        )

    def owned(at, slot):
        _, group, _, per, shift = plan[at]
        mine = lax.rem(me, group)
        head = lax.rem(mine + group - shift, group) * per + slot
        return head, mine

    for at in order:
        _, group, rows, per, _ = plan[at]
        for slot in range(per):
            head, mine = owned(at, slot)

            @pl.when(head < heads)
            def _(at=at, group=group, rows=rows, slot=slot, head=head, mine=mine):
                arrived = inbox[at].at[slot, pl.ds(0, group - 1)]
                pltpu.make_async_copy(arrived, arrived, recv_sem.at[at, slot]).wait()
                block = inbox[at][slot].reshape(tokens, 2 * pair)
                left = block[:, :pair].astype(jnp.float32)
                query = jnp.where(low, left, 0.0).astype(jnp.bfloat16)
                key = swap_halves(left).astype(jnp.bfloat16)
                got, peak = causal_unit(query, key, block[:, pair:].astype(jnp.bfloat16))
                lse = peak + jnp.log(jnp.where(low, 1.0, got))
                hi = lse.astype(jnp.bfloat16).astype(jnp.float32)
                rest = lse - hi
                mid = rest.astype(jnp.bfloat16).astype(jnp.float32)
                parts = jnp.where(lane == mid_lane, hi, 0.0)
                parts = jnp.where(lane == mid_lane + 1, mid, parts)
                parts = jnp.where(lane == mid_lane + 2, rest - mid, parts)
                result = jnp.where(low, got / jnp.where(low, swap_halves(got), 1.0), parts)
                outbox[at][slot] = result.reshape(group, rows, pair).astype(outbox[at].dtype)

                def give(step, carry):
                    returning(at, slot, head, lax.rem(mine + step, group)).start()
                    return carry

                lax.fori_loop(1, group, give, 0)
                back[at][head] = outbox[at][slot, mine]

    def collect(at):
        def one(head, carry):
            _, own, mine, slot = place(plan[at], head)

            @pl.when(jnp.logical_not(own))
            def _():
                sending(at, head).wait_send()
                returning(at, slot, head, mine).wait_recv()

            return carry

        lax.fori_loop(0, heads, one, 0)

    for at in order:
        collect(at)

    token = lax.broadcasted_iota(jnp.int32, (tokens, 1), 0)

    def merge(p, carry):
        cols = pl.ds(pl.multiple_of(p * pair, pair), pair)
        values, lses = [], []
        for at, (height, group, rows, _, _) in enumerate(plan):
            spread = lax.broadcasted_iota(jnp.int32, (tokens, rows), 0)
            source = lax.broadcasted_iota(jnp.int32, (tokens, rows), 1)
            got, lse = [], []
            for side in range(2):
                head = 2 * p + side
                offset = offs[height, head]
                hit = jnp.where(spread == source * group + offset, 1.0, 0.0).astype(jnp.bfloat16)
                sent = back[at][head]
                if side == 1:
                    sent = swap_halves(sent)
                moved = jnp.dot(hit, sent.astype(jnp.bfloat16), preferred_element_type=jnp.float32)
                other = jnp.logical_not(low) if side == 0 else low
                level_lse = jnp.sum(jnp.where(other, moved, 0.0), axis=1, keepdims=True)
                kept = lax.rem(token, group) == offset
                lse.append(jnp.where(kept, level_lse, -1e30))
                got.append(moved)
            values.append(jnp.where(low, got[0], got[1]))
            lses.append(jnp.where(low, lse[0], lse[1]))
        best = peaks[:, cols]
        for lse in lses:
            best = jnp.maximum(best, lse)
        keep = jnp.exp(peaks[:, cols] - best)
        top = numer[:, cols] * keep
        bottom = total[:, cols] * keep
        for value, lse in zip(values, lses):
            share = jnp.exp(lse - best)
            top = top + value * share
            bottom = bottom + share
        out_ref[:, cols] = (top / bottom).astype(out_ref.dtype)
        return carry

    lax.fori_loop(0, pairs, merge, 0)

    for at in order:
        _, group, _, per, _ = plan[at]
        for slot in range(per):
            head, _ = owned(at, slot)

            @pl.when(head < heads)
            def _(at=at, group=group, slot=slot):
                gone = outbox[at].at[slot, pl.ds(0, group - 1)]
                pltpu.make_async_copy(gone, gone, ret_send.at[at, slot]).wait()


def exchange_body(queries, keys, values, offsets):
    tokens, model = queries.shape
    levels, heads = offsets.shape
    count = lax.axis_size("ctx")
    plan = plan_of(levels, count, tokens, heads)
    pair = 2 * (model // heads)
    number = len(plan)
    most = max(entry[3] for entry in plan)

    def dtype(rows):
        return jnp.bfloat16 if rows % 8 == 0 else jnp.float32

    scratch = []
    for _, group, rows, per, _ in plan:
        scratch.append(pltpu.VMEM((heads, rows, 2 * pair), dtype(rows)))
    for _, group, rows, per, _ in plan:
        scratch.append(pltpu.VMEM((per, group, rows, 2 * pair), dtype(rows)))
    for _, group, rows, per, _ in plan:
        scratch.append(pltpu.VMEM((per, group, rows, pair), dtype(rows)))
    for _, group, rows, per, _ in plan:
        scratch.append(pltpu.VMEM((heads, rows, pair), dtype(rows)))
    scratch += [pltpu.VMEM((tokens, model), jnp.float32)] * 3
    scratch += [
        pltpu.SemaphoreType.DMA((number, heads)),
        pltpu.SemaphoreType.DMA((number, most)),
        pltpu.SemaphoreType.DMA((number, most)),
        pltpu.SemaphoreType.DMA((number, heads)),
    ]
    scale = (model // heads) ** -0.5
    vmem = pl.BlockSpec(memory_space=pltpu.VMEM)
    return pl.pallas_call(
        functools.partial(exchange_kernel, plan, heads, scale),
        out_shape=jax.ShapeDtypeStruct((tokens, model), jnp.bfloat16),
        in_specs=[pl.BlockSpec(memory_space=pltpu.SMEM), vmem, vmem, vmem],
        out_specs=vmem,
        scratch_shapes=scratch,
        compiler_params=pltpu.CompilerParams(collective_id=0, has_side_effects=True),
    )(offsets, queries, keys, values)


def solution(mesh):
    in_specs = (P("ctx", None), P("ctx", None), P("ctx", None), P())
    out_specs = P("ctx", None)
    return jax.shard_map(
        exchange_body, mesh=mesh, in_specs=in_specs, out_specs=out_specs, check_vma=False
    )
```

```python
import functools

import jax
import jax.numpy as jnp
from jax import lax
from jax.experimental import pallas as pl
from jax.experimental.pallas import tpu as pltpu
from jax.sharding import PartitionSpec as P

MESH = pl.DeviceIdType.MESH


def plan_of(levels, count, tokens, heads):
    plan = []
    late = False
    for height in range(1, levels):
        group = min(4**height, count)
        per = -(-heads // group)
        shift = 0
        if group >= 2 * heads:
            shift = group // 4 + (group // 2 - heads if late else 0)
            late = not late
        plan.append((height, group, tokens // group, per, shift))
    return plan


def is_packed(rows):
    return rows % 32 == 0


def halves(shape):
    return lax.broadcasted_iota(jnp.int32, shape, 1) < shape[1] // 2


def swap_halves(value):
    return pltpu.roll(value.astype(jnp.float32), value.shape[1] // 2, 1)


def causal_unit(query, key, value):
    tokens = query.shape[0]
    half = tokens // 2
    outs, peaks = [], []
    for start in (0, half):
        end = start + half
        scores = lax.dot_general(
            query[start:end],
            key[:end],
            (((1,), (1,)), ((), ())),
            preferred_element_type=jnp.float32,
        )
        rows = lax.broadcasted_iota(jnp.int32, scores.shape, 0) + start
        cols = lax.broadcasted_iota(jnp.int32, scores.shape, 1)
        scores = jnp.where(cols <= rows, scores, -1e30)
        peak = jnp.max(scores, axis=1, keepdims=True)
        weights = jnp.exp(scores - peak).astype(jnp.bfloat16)
        outs.append(jnp.dot(weights, value[:end], preferred_element_type=jnp.float32))
        peaks.append(peak)
    return jnp.concatenate(outs, 0), jnp.concatenate(peaks, 0)


def exchange_kernel(plan, heads, scale, offs, q_ref, k_ref, v_ref, out_ref, *scratch):
    number = len(plan)
    stage = scratch[:number]
    inbox = scratch[number : 2 * number]
    outbox = scratch[2 * number : 3 * number]
    back = scratch[3 * number : 4 * number]
    numer, total, peaks, send_sem, recv_sem, ret_send, ret_recv = scratch[4 * number :]
    tokens = q_ref.shape[0]
    pair = 2 * (q_ref.shape[1] // heads)
    pairs = heads // 2
    me = lax.axis_index("ctx")
    count = lax.axis_size("ctx")

    barrier = pltpu.get_barrier_semaphore()

    def owns(device, entry):
        _, group, _, per, shift = entry
        return lax.rem(lax.rem(device, group) + group - shift, group) * per < heads

    def greet(step, carry):
        other = lax.rem(me + step, count)
        meets = False
        for entry in plan:
            group = entry[1]
            same = lax.div(me, group) == lax.div(other, group)
            meets = jnp.logical_or(
                meets, jnp.logical_and(same, jnp.logical_or(owns(me, entry), owns(other, entry)))
            )

        @pl.when(meets)
        def _():
            pl.semaphore_signal(barrier, inc=1, device_id=(other,), device_id_type=MESH)

        return carry + jnp.where(meets, 1, 0)

    partners = lax.fori_loop(1, count, greet, 0)

    picked = sum(rows for _, _, rows, _, _ in plan)
    row_id = lax.broadcasted_iota(jnp.int32, (picked, tokens), 0)
    col_id = lax.broadcasted_iota(jnp.int32, (picked, tokens), 1)
    low_p = halves((picked, pair))

    def pick(p, carry):
        cols = pl.ds(pl.multiple_of(p * pair, pair), pair)
        packed = jnp.concatenate([q_ref[:, cols], k_ref[:, cols], v_ref[:, cols]], 1)
        for side in range(2):
            head = 2 * p + side
            first = 0
            target = jnp.zeros((picked, tokens), jnp.int32)
            for height, group, rows, _, _ in plan:
                here = (row_id - first) * group + offs[height, head]
                target = here if first == 0 else jnp.where(row_id < first, target, here)
                first += rows
            hit = jnp.where(col_id == target, 1.0, 0.0).astype(jnp.bfloat16)
            got = jnp.dot(hit, packed, preferred_element_type=jnp.float32)
            query, key, value = got[:, :pair], got[:, pair : 2 * pair], got[:, 2 * pair :]
            swapped = swap_halves(value)
            if side == 0:
                key = swap_halves(key)
            else:
                query = swap_halves(query)
                value, swapped = swapped, value
            left = jnp.where(low_p, query * scale, key)
            first = 0
            for at, (_, _, rows, _, _) in enumerate(plan):
                kind = stage[at].dtype
                last = first + rows
                if is_packed(rows):
                    middle = first + rows // 2
                    right = jnp.where(
                        low_p[: rows // 2], value[first:middle], swapped[middle:last]
                    )
                    stage[at][head] = jnp.concatenate([left[first:last], right], 0).astype(kind)
                else:
                    stage[at][head] = jnp.concatenate(
                        [left[first:last], value[first:last]], 1
                    ).astype(kind)
                first = last
        return carry

    lax.fori_loop(0, pairs, pick, 0)
    pl.semaphore_wait(barrier, partners)

    def place(entry, head):
        _, group, _, per, shift = entry
        where = lax.rem(shift + head // per, group)
        mine = lax.rem(me, group)
        return me - mine + where, where == mine, mine, head % per

    def sending(at, head):
        owner, _, mine, slot = place(plan[at], head)
        return pltpu.make_async_remote_copy(
            src_ref=stage[at].at[head],
            dst_ref=inbox[at].at[slot, mine],
            send_sem=send_sem.at[at, head],
            recv_sem=recv_sem.at[at, slot],
            device_id=(owner,),
            device_id_type=MESH,
        )

    order = list(range(number))[::-1]
    for at in order:

        def push(head, carry, at=at):
            _, own, mine, slot = place(plan[at], head)

            @pl.when(jnp.logical_not(own))
            def _():
                sending(at, head).start()

            @pl.when(own)
            def _():
                inbox[at][slot, mine] = stage[at][head]

            return carry

        lax.fori_loop(0, heads, push, 0)

    low = halves((tokens, pair))

    def base(p, carry):
        cols = pl.ds(pl.multiple_of(p * pair, pair), pair)
        query = q_ref[:, cols].astype(jnp.float32) * scale
        key = k_ref[:, cols]
        value = v_ref[:, cols].astype(jnp.float32)
        got = []
        for side in range(2):
            mask = low if side == 0 else jnp.logical_not(low)
            got.append(
                causal_unit(
                    jnp.where(mask, query, 0.0).astype(jnp.bfloat16),
                    key,
                    jnp.where(mask, value, 1.0).astype(jnp.bfloat16),
                )
            )
        numer[:, cols] = jnp.where(low, got[0][0], got[1][0])
        total[:, cols] = swap_halves(jnp.where(low, got[1][0], got[0][0]))
        peaks[:, cols] = jnp.where(low, got[0][1], got[1][1])
        return carry

    lax.fori_loop(0, 2 * pairs // 3, base, 0)

    lane = lax.broadcasted_iota(jnp.int32, (tokens, pair), 1)
    mid_lane = pair // 2

    def returning(at, slot, head, there):
        _, group, _, _, _ = plan[at]
        mine = lax.rem(me, group)
        return pltpu.make_async_remote_copy(
            src_ref=outbox[at].at[slot, there],
            dst_ref=back[at].at[head],
            send_sem=ret_send.at[at, slot],
            recv_sem=ret_recv.at[at, head],
            device_id=(me - mine + there,),
            device_id_type=MESH,
        )

    def owned(at, slot):
        _, group, _, per, shift = plan[at]
        mine = lax.rem(me, group)
        head = lax.rem(mine + group - shift, group) * per + slot
        return head, mine

    for at in order:
        _, group, rows, per, _ = plan[at]
        for slot in range(per):
            head, mine = owned(at, slot)

            @pl.when(head < heads)
            def _(at=at, group=group, rows=rows, slot=slot, head=head, mine=mine):
                arrived = inbox[at].at[slot, pl.ds(0, group - 1)]
                pltpu.make_async_copy(arrived, arrived, recv_sem.at[at, slot]).wait()
                block = inbox[at][slot]
                if is_packed(rows):
                    left = block[:, :rows].reshape(tokens, pair).astype(jnp.float32)
                    right = block[:, rows:].reshape(tokens // 2, pair).astype(jnp.float32)
                    split = (group, rows // 2, pair)
                    right = jnp.concatenate(
                        [right.reshape(split), swap_halves(right).reshape(split)], 1
                    ).reshape(tokens, pair)
                else:
                    block = block.reshape(tokens, 2 * pair)
                    left = block[:, :pair].astype(jnp.float32)
                    right = block[:, pair:].astype(jnp.float32)
                value = jnp.where(low, right, 1.0).astype(jnp.bfloat16)
                query = jnp.where(low, left, 0.0).astype(jnp.bfloat16)
                key = swap_halves(left).astype(jnp.bfloat16)
                got, peak = causal_unit(query, key, value)
                lse = peak + jnp.log(jnp.where(low, 1.0, got))
                hi = lse.astype(jnp.bfloat16).astype(jnp.float32)
                rest = lse - hi
                mid = rest.astype(jnp.bfloat16).astype(jnp.float32)
                parts = jnp.where(lane == mid_lane, hi, 0.0)
                parts = jnp.where(lane == mid_lane + 1, mid, parts)
                parts = jnp.where(lane == mid_lane + 2, rest - mid, parts)
                result = jnp.where(low, got / jnp.where(low, swap_halves(got), 1.0), parts)
                outbox[at][slot] = result.reshape(group, rows, pair).astype(outbox[at].dtype)

                def give(step, carry):
                    returning(at, slot, head, lax.rem(mine + step, group)).start()
                    return carry

                lax.fori_loop(1, group, give, 0)
                back[at][head] = outbox[at][slot, mine]

    lax.fori_loop(2 * pairs // 3, pairs, base, 0)

    def collect(at):
        def one(head, carry):
            _, own, mine, slot = place(plan[at], head)

            @pl.when(jnp.logical_not(own))
            def _():
                sending(at, head).wait_send()
                returning(at, slot, head, mine).wait_recv()

            return carry

        lax.fori_loop(0, heads, one, 0)

    for at in order:
        collect(at)

    token = lax.broadcasted_iota(jnp.int32, (tokens, 1), 0)

    def merge(p, carry):
        cols = pl.ds(pl.multiple_of(p * pair, pair), pair)
        values, lses = [], []
        for at, (height, group, rows, _, _) in enumerate(plan):
            spread = lax.broadcasted_iota(jnp.int32, (tokens, rows), 0)
            source = lax.broadcasted_iota(jnp.int32, (tokens, rows), 1)
            got, lse = [], []
            for side in range(2):
                head = 2 * p + side
                offset = offs[height, head]
                hit = jnp.where(spread == source * group + offset, 1.0, 0.0).astype(jnp.bfloat16)
                sent = back[at][head]
                if side == 1:
                    sent = swap_halves(sent)
                moved = jnp.dot(hit, sent.astype(jnp.bfloat16), preferred_element_type=jnp.float32)
                other = jnp.logical_not(low) if side == 0 else low
                level_lse = jnp.sum(jnp.where(other, moved, 0.0), axis=1, keepdims=True)
                kept = jnp.bitwise_and(token, group - 1) == offset
                lse.append(jnp.where(kept, level_lse, -1e30))
                got.append(moved)
            values.append(jnp.where(low, got[0], got[1]))
            lses.append(jnp.where(low, lse[0], lse[1]))
        best = peaks[:, cols]
        for lse in lses:
            best = jnp.maximum(best, lse)
        keep = jnp.exp(peaks[:, cols] - best)
        top = numer[:, cols] * keep
        bottom = total[:, cols] * keep
        for value, lse in zip(values, lses):
            share = jnp.exp(lse - best)
            top = top + value * share
            bottom = bottom + share
        out_ref[:, cols] = (top / bottom).astype(out_ref.dtype)
        return carry

    lax.fori_loop(0, pairs, merge, 0, unroll=2)

    for at in order:
        _, group, _, per, _ = plan[at]
        for slot in range(per):
            head, _ = owned(at, slot)

            @pl.when(head < heads)
            def _(at=at, group=group, slot=slot):
                gone = outbox[at].at[slot, pl.ds(0, group - 1)]
                pltpu.make_async_copy(gone, gone, ret_send.at[at, slot]).wait()


def exchange_body(queries, keys, values, offsets):
    tokens, model = queries.shape
    levels, heads = offsets.shape
    count = lax.axis_size("ctx")
    plan = plan_of(levels, count, tokens, heads)
    pair = 2 * (model // heads)
    number = len(plan)
    most = max(entry[3] for entry in plan)

    def dtype(rows):
        return jnp.bfloat16 if rows % 8 == 0 else jnp.float32

    def block(rows):
        return (rows + rows // 2, pair) if is_packed(rows) else (rows, 2 * pair)

    scratch = []
    for _, group, rows, per, _ in plan:
        scratch.append(pltpu.VMEM((heads, *block(rows)), dtype(rows)))
    for _, group, rows, per, _ in plan:
        scratch.append(pltpu.VMEM((per, group, *block(rows)), dtype(rows)))
    for _, group, rows, per, _ in plan:
        scratch.append(pltpu.VMEM((per, group, rows, pair), dtype(rows)))
    for _, group, rows, per, _ in plan:
        scratch.append(pltpu.VMEM((heads, rows, pair), dtype(rows)))
    scratch += [pltpu.VMEM((tokens, model), jnp.float32)] * 3
    scratch += [
        pltpu.SemaphoreType.DMA((number, heads)),
        pltpu.SemaphoreType.DMA((number, most)),
        pltpu.SemaphoreType.DMA((number, most)),
        pltpu.SemaphoreType.DMA((number, heads)),
    ]
    scale = (model // heads) ** -0.5
    vmem = pl.BlockSpec(memory_space=pltpu.VMEM)
    return pl.pallas_call(
        functools.partial(exchange_kernel, plan, heads, scale),
        out_shape=jax.ShapeDtypeStruct((tokens, model), jnp.bfloat16),
        in_specs=[pl.BlockSpec(memory_space=pltpu.SMEM), vmem, vmem, vmem],
        out_specs=vmem,
        scratch_shapes=scratch,
        compiler_params=pltpu.CompilerParams(collective_id=0, has_side_effects=True),
    )(offsets, queries, keys, values)


def solution(mesh):
    in_specs = (P("ctx", None), P("ctx", None), P("ctx", None), P())
    out_specs = P("ctx", None)
    return jax.shard_map(
        exchange_body, mesh=mesh, in_specs=in_specs, out_specs=out_specs, check_vma=False
    )
```
